32 devices in a mesh: rows: 16 (over z, y, x), feat: 2 (over core).
Axes of the slice: x: 2, y: 2, z: 4, core: 2. Of those that a mesh axis runs over, the one named last changes fastest.
Arguments:
- bin_words: int32 [32768, 128], P('rows', 'feat'), may hold values from -2147483648 to 2147483646, as said below
- gradient: bfloat16 [32768], P('rows'), may hold values from -6 to 6
- hessian: bfloat16 [32768], P('rows'), may hold values from 0.099609375 to 1
- leaf_id: int32 [32768], P('rows'), may hold values from 0 to 63
- small_side: int32 [32], replicated, may hold values from 0 to 1
- parent_hist: float32 [512, 64, 256], P(('feat', 'rows')), may hold values from -12 to 12
Outputs:
- smaller_hist: float32 [512, 64, 256], P(('feat', 'rows'))
- larger_hist: float32 [512, 64, 256], P(('feat', 'rows'))
- feature_gain: float32 [512, 32], P(('feat', 'rows'))
- best_gain: float32 [32], replicated
The draws below stay inside these ranges and needn't reach their ends.
Inputs may be any that keep to these rules, and one draw needn't show every extreme that they name: `bin_words`: byte k of word w (bits 8 k to 8 k + 7) holds the code of feature 4 w + k; a feature's bin is that byte modulo 256.
All inputs are finite; a program needn't handle non-finite values.
Results may differ from the reference program's by a relative error of at most 0.0003.
Values may be sent and summed in bfloat16 or wider, within the bound.
A program may use at most 64 MiB of HBM per device.

```python
import math
import jax
import jax.numpy as jnp
from jax import lax

F = 512
BINS = 256
PAIRS = 32
LEAVES = 64
ROWS = 32768


def draw_bin_words(key, part):
    return jax.random.randint(jax.random.fold_in(key, 11), (ROWS, F // 4), -2147483648, 2147483647, dtype=jnp.int32)


def touch_ends(result, key, smallest, high):
    longest = result.shape.index(max(result.shape))
    spots = []
    for shift in (0, 1):
        where = [jax.random.randint(jax.random.fold_in(key, axis), (), 0, length) for axis, length in enumerate(result.shape)]
        where[longest] = (where[longest] + shift) % result.shape[longest]
        spots.append(tuple(where))
    return result.at[spots[0]].set(smallest).at[spots[1]].set(high)


def steps_of(rng, dims, cuts, smallest, top_value):
    factor_of, own = 1.0, jax.random.fold_in(rng, 6)
    for position, parts in cuts:
        draws = jnp.exp(jax.random.uniform(jax.random.fold_in(own, position), (parts,), jnp.float32, smallest / len(cuts), top_value / len(cuts)))
        factor_of = factor_of * jnp.repeat(draws, dims[position] // parts).reshape([-1 if axis == position else 1 for axis in range(len(dims))])
    return factor_of


def centred(rng, extent, deviation, bound, cuts=(), kind=jnp.bfloat16):
    drawn = deviation * jax.random.normal(rng, extent, jnp.float32)
    if cuts:
        drawn = drawn * steps_of(rng, extent, cuts, -0.22, 0.18)
    return jnp.clip(drawn, -bound, bound).astype(kind)


def setup_inputs(seed: int = 0) -> dict:
    key_of = jax.random.split(jax.random.key(seed), 7)
    return {
        "bin_words": draw_bin_words(jax.random.fold_in(key_of[6], 71), 0),
        "gradient": centred(key_of[1], (ROWS,), 1.0, 6.0, ((0, 16),)),
        "hessian": jnp.clip(jnp.exp(math.log(1.0) - 2.306499 * jax.random.uniform(key_of[2], (ROWS,), jnp.float32) ** steps_of(key_of[2], (ROWS,), ((0, 16),), -0.2, 0.2)), 0.099609375, 1.0).astype(jnp.bfloat16),
        "leaf_id": touch_ends(jax.random.randint(key_of[3], (ROWS,), 0, LEAVES), jax.random.fold_in(key_of[3], 1), 0, LEAVES - 1).astype(jnp.int32),
        "small_side": touch_ends(jax.random.randint(key_of[4], (PAIRS,), 0, 2), jax.random.fold_in(key_of[4], 1), 0, 1).astype(jnp.int32),
        "parent_hist": centred(key_of[5], (F, 2 * PAIRS, BINS), 2.0, 12.0, ((0, 32),), jnp.float32),
    }


ridge_term = 1.0


def unpack_bins(bin_words, bin_count):
    shifts = 8 * jnp.arange(4, dtype=jnp.int32)
    shifted = jnp.right_shift(bin_words[:, :, None], shifts[None, None, :])
    bin_codes = jnp.bitwise_and(shifted, bin_count - 1)
    return bin_codes.reshape(bin_words.shape[0], bin_words.shape[1] * 4)


def row_weights(gradient, hessian, leaf_id, small_side):
    pair_ids = jnp.arange(small_side.shape[0], dtype=jnp.int32)
    member = ((leaf_id[:, None] // 2 == pair_ids[None, :]) & (leaf_id[:, None] % 2 == small_side[None, :])).astype(jnp.float32)
    return jnp.concatenate([gradient.astype(jnp.float32)[:, None] * member, hessian.astype(jnp.float32)[:, None] * member], axis=1)


def gains_from_left(left_sums, totals, pair_count):
    grad_left = left_sums[:, :pair_count]
    hess_left = left_sums[:, pair_count:]
    grad_total = totals[:pair_count][None, :, None]
    hess_total = totals[pair_count:][None, :, None]
    split_gain = 0.5 * (grad_left * grad_left / (hess_left + ridge_term)
                        + (grad_total - grad_left) * (grad_total - grad_left) / (hess_total - hess_left + ridge_term)
                        - grad_total * grad_total / (hess_total + ridge_term))
    return jnp.max(split_gain, axis=2)


def reference(bin_words, gradient, hessian, leaf_id, small_side, parent_hist):
    bin_codes = unpack_bins(bin_words, BINS)
    weights = row_weights(gradient, hessian, leaf_id, small_side)

    def one_feature(column):
        return jax.ops.segment_sum(weights, column, num_segments=BINS).T

    smaller_hist = lax.map(one_feature, bin_codes.T)
    larger_hist = parent_hist - smaller_hist
    totals = jnp.sum(weights, axis=0)
    left_sums = jnp.cumsum(smaller_hist, axis=2)[:, :, :BINS - 1]
    feature_gain = gains_from_left(left_sums, totals, PAIRS)
    best_gain = jnp.max(feature_gain, axis=0)
    return (smaller_hist, larger_hist, feature_gain, best_gain)
```

```python
import functools

import jax
import jax.numpy as jnp
from jax import lax
from jax.experimental import pallas as pl
from jax.experimental.pallas import tpu as pltpu
from jax.sharding import PartitionSpec as P

ridge_term = 1.0
MESH = pl.DeviceIdType.MESH
VMEM = pltpu.MemorySpace.VMEM


def gains_from_left(left_sums, totals, pair_count):
    grad_left = left_sums[:, :pair_count]
    hess_left = left_sums[:, pair_count:]
    grad_total = totals[:, :pair_count]
    hess_total = totals[:, pair_count:]
    split_gain = 0.5 * (
        grad_left * grad_left / (hess_left + ridge_term)
        + (grad_total - grad_left)
        * (grad_total - grad_left)
        / (hess_total - hess_left + ridge_term)
        - grad_total * grad_total / (hess_total + ridge_term)
    )
    return jnp.max(split_gain, axis=2)


def exchange_kernel(n, words_ref, vals_ref, words_out, vals_out, send_sem, recv_sem, own_sem):
    me = lax.axis_index("rows")
    barrier = pltpu.get_barrier_semaphore()

    def greet(d, carry):
        peer = lax.rem(me + d, n)
        pl.semaphore_signal(barrier, inc=1, device_id={"rows": peer}, device_id_type=MESH)
        return carry

    lax.fori_loop(1, n, greet, 0)
    own_words = pltpu.make_async_copy(words_ref.at[me], words_out.at[me], own_sem.at[0])
    own_vals = pltpu.make_async_copy(vals_ref, vals_out.at[me], own_sem.at[1])
    own_words.start()
    own_vals.start()
    pl.semaphore_wait(barrier, n - 1)

    def copies(peer, slot):
        words = pltpu.make_async_remote_copy(
            src_ref=words_ref.at[peer],
            dst_ref=words_out.at[slot],
            send_sem=send_sem.at[0, peer],
            recv_sem=recv_sem.at[0, slot],
            device_id={"rows": peer},
            device_id_type=MESH,
        )
        vals = pltpu.make_async_remote_copy(
            src_ref=vals_ref,
            dst_ref=vals_out.at[slot],
            send_sem=send_sem.at[1, peer],
            recv_sem=recv_sem.at[1, slot],
            device_id={"rows": peer},
            device_id_type=MESH,
        )
        return words, vals

    def send(d, carry):
        words, vals = copies(lax.rem(me + d, n), me)
        words.start()
        vals.start()
        return carry

    lax.fori_loop(1, n, send, 0)
    own_words.wait()
    own_vals.wait()

    def finish(d, carry):
        peer = lax.rem(me + d, n)
        words, vals = copies(peer, peer)
        words.wait()
        vals.wait()
        return carry

    lax.fori_loop(1, n, finish, 0)


def exchange(words, vals, n):
    return pl.pallas_call(
        functools.partial(exchange_kernel, n),
        out_shape=(
            jax.ShapeDtypeStruct(words.shape, words.dtype),
            jax.ShapeDtypeStruct((n,) + vals.shape, vals.dtype),
        ),
        in_specs=[pl.BlockSpec(memory_space=VMEM)] * 2,
        out_specs=[pl.BlockSpec(memory_space=VMEM)] * 2,
        scratch_shapes=[
            pltpu.SemaphoreType.DMA((2, n)),
            pltpu.SemaphoreType.DMA((2, n)),
            pltpu.SemaphoreType.DMA((2,)),
        ],
        compiler_params=pltpu.CompilerParams(collective_id=0, has_side_effects=True),
        name="exchange",
    )(words, vals)


def add_block(words, vals, hist_ref, bins, weights, lanes_of, half, pairs):
    f32, bf16 = jnp.float32, jnp.bfloat16
    rows = words.shape[1]
    per_word = bins.shape[0] // words.shape[0]
    words_count = words.shape[0]
    for k in range(per_word):
        code = jnp.bitwise_and(jnp.right_shift(words, 8 * k), 2 * half - 1)
        bins[k * words_count : (k + 1) * words_count, :] = code.astype(f32)
    vals = vals.astype(f32)
    pair_row = jnp.broadcast_to(vals[2:3, :], (pairs, rows))
    member = pair_row == lax.broadcasted_iota(jnp.int32, (pairs, rows), 0).astype(f32)
    for c in range(2):
        column = jnp.broadcast_to(vals[c : c + 1, :], (pairs, rows))
        weights[c * pairs : (c + 1) * pairs, :] = jnp.where(member, column, 0.0).astype(bf16)

    def one_feature(w, k):
        row = jnp.broadcast_to(bins[pl.ds(k * words_count + w, 1), :], (16, rows))
        upper = row >= half
        low = jnp.where(upper, row - half, row).astype(bf16)
        top = jnp.where(upper, 1.0, 0.0).astype(bf16)
        low = jnp.concatenate([low] * (half // 16), axis=0)
        top = jnp.concatenate([top] * (2 * pairs // 16), axis=0)
        one_hot = jnp.where(low == lanes_of[...], jnp.bfloat16(1), jnp.bfloat16(0))
        held = weights[...]
        is_top = top > jnp.bfloat16(0.5)
        zero = jnp.zeros_like(held)
        split = jnp.concatenate(
            [jnp.where(is_top, zero, held), jnp.where(is_top, held, zero)], axis=0
        )
        part = lax.dot_general(
            split, one_hot, (((1,), (1,)), ((), ())), preferred_element_type=f32
        )
        f = w * per_word + k
        hist_ref[f, :, :half] += part[: 2 * pairs]
        hist_ref[f, :, half:] += part[2 * pairs :]

    def one_word(w, carry):
        for k in range(per_word):
            one_feature(w, k)
        return carry

    lax.fori_loop(0, words_count, one_word, 0)


def fill_lanes(lanes_of):
    lanes_of[...] = (
        lax.broadcasted_iota(jnp.int32, lanes_of.shape, 0).astype(jnp.float32).astype(jnp.bfloat16)
    )


def histogram_kernel(n, half, pairs, words_ref, vals_ref, hist_ref, bins, weights, lanes_of):
    fill_lanes(lanes_of)
    hist_ref[...] = jnp.zeros_like(hist_ref)

    def block(s, carry):
        add_block(words_ref[s], vals_ref[s], hist_ref, bins, weights, lanes_of, half, pairs)
        return carry

    lax.fori_loop(0, n, block, 0)


def histogram(words, vals, pairs, bin_count):
    n, word_count, rows = words.shape
    features = word_count * 4
    half = bin_count // 2
    return pl.pallas_call(
        functools.partial(histogram_kernel, n, half, pairs),
        out_shape=jax.ShapeDtypeStruct((features, 2 * pairs, bin_count), jnp.float32),
        in_specs=[pl.BlockSpec(memory_space=VMEM)] * 2,
        out_specs=pl.BlockSpec(memory_space=VMEM),
        scratch_shapes=[
            pltpu.VMEM((features, rows), jnp.float32),
            pltpu.VMEM((2 * pairs, rows), jnp.bfloat16),
            pltpu.VMEM((half, rows), jnp.bfloat16),
        ],
        name="histogram",
    )(words, vals)


def maximum_kernel(n, m, best_ref, out_ref, slots, send_sem, recv_sem):
    me = lax.axis_index("rows") * m + lax.axis_index("feat")
    total = n * m
    barrier = pltpu.get_barrier_semaphore()

    def place(d):
        peer = lax.rem(me + d, total)
        return peer, {"rows": peer // m, "feat": lax.rem(peer, m)}

    def greet(d, carry):
        pl.semaphore_signal(barrier, inc=1, device_id=place(d)[1], device_id_type=MESH)
        return carry

    lax.fori_loop(1, total, greet, 0)
    pl.semaphore_wait(barrier, total - 1)

    def copy(d, slot):
        peer, where = place(d)
        return pltpu.make_async_remote_copy(
            src_ref=best_ref,
            dst_ref=slots.at[me if slot is None else slot],
            send_sem=send_sem.at[peer],
            recv_sem=recv_sem.at[me if slot is None else slot],
            device_id=where,
            device_id_type=MESH,
        )

    def send(d, carry):
        copy(d, None).start()
        return carry

    lax.fori_loop(1, total, send, 0)

    def finish(d, best):
        peer, _ = place(d)
        copy(d, peer).wait()
        return jnp.maximum(best, slots[peer])

    out_ref[...] = lax.fori_loop(1, total, finish, best_ref[...])


def all_maximum(best, n, m):
    return pl.pallas_call(
        functools.partial(maximum_kernel, n, m),
        out_shape=jax.ShapeDtypeStruct(best.shape, best.dtype),
        in_specs=[pl.BlockSpec(memory_space=VMEM)],
        out_specs=pl.BlockSpec(memory_space=VMEM),
        scratch_shapes=[
            pltpu.VMEM((n * m,) + best.shape, best.dtype),
            pltpu.SemaphoreType.DMA((n * m,)),
            pltpu.SemaphoreType.DMA((n * m,)),
        ],
        compiler_params=pltpu.CompilerParams(collective_id=1, has_side_effects=True),
        name="maximum",
    )(best)


def on_device(bin_words, gradient, hessian, leaf_id, small_side, parent_hist):
    pair_count = small_side.shape[0]
    bin_count = parent_hist.shape[2]
    n = lax.axis_size("rows")
    m = lax.axis_size("feat")
    rows, word_count = bin_words.shape
    words = bin_words.T.reshape(n, word_count // n, rows)
    pair_ids = jnp.arange(pair_count, dtype=jnp.int32)
    is_member = jnp.any(
        (pair_ids * 2 + small_side)[:, None] == leaf_id[None, :], axis=0
    )
    pair = jnp.where(is_member, leaf_id // 2, pair_count).astype(jnp.bfloat16)
    vals = jnp.stack([gradient, hessian, pair, jnp.zeros_like(gradient)])
    moved_words, moved_vals = exchange(words, vals, n)
    local_hist = histogram(moved_words, moved_vals, pair_count, bin_count)
    upper = (
        lax.iota(jnp.int32, bin_count)[:, None] <= lax.iota(jnp.int32, bin_count)[None, :]
    ).astype(jnp.float32)
    sums = jnp.einsum("fcb,bt->fct", local_hist, upper, precision=lax.Precision.HIGHEST)
    feature_gain = gains_from_left(sums[:, :, :-1], sums[:, :, -1:], pair_count)
    best = jnp.pad(jnp.max(feature_gain, axis=0), (0, 128 - pair_count))[None, :]
    best_gain = all_maximum(best, n, m)[0, :pair_count]
    return (local_hist, parent_hist - local_hist, feature_gain, best_gain)


def solution(mesh):
    placed = (
        P("rows", "feat"),
        P("rows"),
        P("rows"),
        P("rows"),
        P(),
        P(("feat", "rows"), None, None),
    )
    return jax.shard_map(
        on_device,
        mesh=mesh,
        in_specs=placed,
        out_specs=(
            P(("feat", "rows"), None, None),
            P(("feat", "rows"), None, None),
            P(("feat", "rows"), None),
            P(),
        ),
        check_vma=False,
    )
```

```python
import functools

import jax
import jax.numpy as jnp
from jax import lax
from jax.experimental import pallas as pl
from jax.experimental.pallas import tpu as pltpu
from jax.sharding import PartitionSpec as P

ridge_term = 1.0
MESH = pl.DeviceIdType.MESH
VMEM = pltpu.MemorySpace.VMEM


def gains_from_left(left, pairs):
    grad_left, hess_left = left[:pairs], left[pairs:]
    last = left.shape[1] - 1
    grad_total, hess_total = grad_left[:, last:], hess_left[:, last:]
    gain = 0.5 * (
        grad_left * grad_left / (hess_left + ridge_term)
        + (grad_total - grad_left)
        * (grad_total - grad_left)
        / (hess_total - hess_left + ridge_term)
        - grad_total * grad_total / (hess_total + ridge_term)
    )
    lane = lax.broadcasted_iota(jnp.int32, gain.shape, 1)
    gain = jnp.where(lane < last, gain, -jnp.inf)
    best = gain[:, :128]
    for first in range(128, last + 1, 128):
        best = jnp.maximum(best, gain[:, first : first + 128])
    return best


def add_block(words, vals, hist_ref, bins, weights, lanes_of, half, pairs):
    f32, bf16 = jnp.float32, jnp.bfloat16
    rows = words.shape[1]
    per_word = bins.shape[0] // words.shape[0]
    words_count = words.shape[0]
    for k in range(per_word):
        code = jnp.bitwise_and(jnp.right_shift(words, 8 * k), 2 * half - 1)
        bins[k * words_count : (k + 1) * words_count, :] = code.astype(f32)
    vals = vals.astype(f32)
    pair_row = jnp.broadcast_to(vals[2:3, :], (pairs, rows))
    member = pair_row == lax.broadcasted_iota(jnp.int32, (pairs, rows), 0).astype(f32)
    for c in range(2):
        column = jnp.broadcast_to(vals[c : c + 1, :], (pairs, rows))
        weights[c * pairs : (c + 1) * pairs, :] = jnp.where(member, column, 0.0).astype(bf16)

    def one_feature(w, k):
        row = jnp.broadcast_to(bins[pl.ds(k * words_count + w, 1), :], (16, rows))
        upper = row >= half
        low = jnp.where(upper, row - half, row).astype(bf16)
        top = jnp.where(upper, 1.0, 0.0).astype(bf16)
        low = jnp.concatenate([low] * (half // 16), axis=0)
        top = jnp.concatenate([top] * (2 * pairs // 16), axis=0)
        one_hot = jnp.where(low == lanes_of[...], jnp.bfloat16(1), jnp.bfloat16(0))
        held = weights[...]
        is_top = top > jnp.bfloat16(0.5)
        zero = jnp.zeros_like(held)
        split = jnp.concatenate(
            [jnp.where(is_top, zero, held), jnp.where(is_top, held, zero)], axis=0
        )
        part = lax.dot_general(
            split, one_hot, (((1,), (1,)), ((), ())), preferred_element_type=f32
        )
        f = w * per_word + k
        hist_ref[f, :, :half] += part[: 2 * pairs]
        hist_ref[f, :, half:] += part[2 * pairs :]

    def one_word(w, carry):
        for k in range(per_word):
            one_feature(w, k)
        return carry

    lax.fori_loop(0, words_count, one_word, 0)


def fill_lanes(lanes_of):
    lanes_of[...] = (
        lax.broadcasted_iota(jnp.int32, lanes_of.shape, 0).astype(jnp.float32).astype(jnp.bfloat16)
    )


def histogram_kernel(
    n, m, half, pairs, words_ref, vals_ref, hist_ref, gain_ref, best_ref,
    words_in, vals_in, bins, weights, lanes_of, send_sem, recv_sem,
    best_own, best_in, best_send, best_recv,
):
    me = lax.axis_index("rows")
    place = me * m + lax.axis_index("feat")
    total = n * m
    barrier = pltpu.get_barrier_semaphore()

    def other(d):
        peer = lax.rem(place + d, total)
        return peer, {"rows": peer // m, "feat": lax.rem(peer, m)}

    def greet(d, carry):
        pl.semaphore_signal(barrier, inc=1, device_id=other(d)[1], device_id_type=MESH)
        return carry

    lax.fori_loop(1, total, greet, 0)

    def copies(peer, slot):
        words = pltpu.make_async_remote_copy(
            src_ref=words_ref.at[peer],
            dst_ref=words_in.at[slot],
            send_sem=send_sem.at[0, peer],
            recv_sem=recv_sem.at[0, slot],
            device_id={"rows": peer},
            device_id_type=MESH,
        )
        vals = pltpu.make_async_remote_copy(
            src_ref=vals_ref,
            dst_ref=vals_in.at[slot],
            send_sem=send_sem.at[1, peer],
            recv_sem=recv_sem.at[1, slot],
            device_id={"rows": peer},
            device_id_type=MESH,
        )
        return words, vals

    pl.semaphore_wait(barrier, total - 1)

    def send(d, carry):
        words, vals = copies(lax.rem(me + d, n), me)
        words.start()
        vals.start()
        return carry

    lax.fori_loop(1, n, send, 0)
    fill_lanes(lanes_of)
    hist_ref[...] = jnp.zeros_like(hist_ref)
    words_in[me] = words_ref[me]
    vals_in[me] = vals_ref[...]

    def block(d, carry):
        source = lax.rem(me - d + n, n)

        @pl.when(d > 0)
        def _():
            words, vals = copies(source, source)
            words.wait_recv()
            vals.wait_recv()

        add_block(words_in[source], vals_in[source], hist_ref, bins, weights, lanes_of, half, pairs)
        return carry

    lax.fori_loop(0, n, block, 0)

    bin_count = 2 * half
    upper = (
        lax.broadcasted_iota(jnp.int32, (bin_count, bin_count), 0)
        <= lax.broadcasted_iota(jnp.int32, (bin_count, bin_count), 1)
    ).astype(jnp.float32)
    per_word = hist_ref.shape[0] // words_ref.shape[1]

    def word_gain(w, carry):
        own = hist_ref[pl.ds(w * per_word, per_word)]
        left = jnp.dot(
            own.reshape(per_word * 2 * pairs, bin_count),
            upper,
            precision=lax.Precision.HIGHEST,
            preferred_element_type=jnp.float32,
        )
        each = [
            gains_from_left(left[k * 2 * pairs : (k + 1) * 2 * pairs], pairs)
            for k in range(per_word)
        ]
        best = jnp.max(jnp.concatenate(each, axis=0).T, axis=0, keepdims=True)
        gain_ref[pl.ds(w, 1), :] = best
        return carry

    lax.fori_loop(0, words_ref.shape[1], word_gain, 0)
    best_own[...] = jnp.max(gain_ref[...], axis=0, keepdims=True)

    def best_copy(d, slot):
        peer, where = other(d)
        return peer, pltpu.make_async_remote_copy(
            src_ref=best_own,
            dst_ref=best_in.at[place if slot is None else slot],
            send_sem=best_send.at[peer],
            recv_sem=best_recv.at[place if slot is None else slot],
            device_id=where,
            device_id_type=MESH,
        )

    def finish(d, carry):
        peer = lax.rem(me + d, n)
        words, vals = copies(peer, peer)
        words.wait_send()
        vals.wait_send()
        return carry

    lax.fori_loop(1, n, finish, 0)

    def best_start(d, carry):
        best_copy(d, None)[1].start()
        return carry

    lax.fori_loop(1, total, best_start, 0)

    def best_finish(d, best):
        peer = lax.rem(place - d + total, total)
        best_copy(total - d, peer)[1].wait()
        return jnp.maximum(best, best_in[peer])

    best_ref[...] = lax.fori_loop(1, total, best_finish, best_own[...])


def histogram(words, vals, pairs, bin_count, m):
    n, word_count, rows = words.shape
    features = word_count * 4
    half = bin_count // 2
    return pl.pallas_call(
        functools.partial(histogram_kernel, n, m, half, pairs),
        out_shape=(
            jax.ShapeDtypeStruct((features, 2 * pairs, bin_count), jnp.float32),
            jax.ShapeDtypeStruct((word_count, 4 * pairs), jnp.float32),
            jax.ShapeDtypeStruct((1, 4 * pairs), jnp.float32),
        ),
        in_specs=[pl.BlockSpec(memory_space=VMEM)] * 2,
        out_specs=[pl.BlockSpec(memory_space=VMEM)] * 3,
        scratch_shapes=[
            pltpu.VMEM(words.shape, words.dtype),
            pltpu.VMEM((n,) + vals.shape, vals.dtype),
            pltpu.VMEM((features, rows), jnp.float32),
            pltpu.VMEM((2 * pairs, rows), jnp.bfloat16),
            pltpu.VMEM((half, rows), jnp.bfloat16),
            pltpu.SemaphoreType.DMA((2, n)),
            pltpu.SemaphoreType.DMA((2, n)),
            pltpu.VMEM((1, 4 * pairs), jnp.float32),
            pltpu.VMEM((n * m, 1, 4 * pairs), jnp.float32),
            pltpu.SemaphoreType.DMA((n * m,)),
            pltpu.SemaphoreType.DMA((n * m,)),
        ],
        compiler_params=pltpu.CompilerParams(collective_id=0, has_side_effects=True),
        name="histogram",
    )(words, vals)


def on_device(bin_words, gradient, hessian, leaf_id, small_side, parent_hist):
    pair_count = small_side.shape[0]
    bin_count = parent_hist.shape[2]
    n = lax.axis_size("rows")
    m = lax.axis_size("feat")
    rows, word_count = bin_words.shape
    words = bin_words.T.reshape(n, word_count // n, rows)
    pair_ids = jnp.arange(pair_count, dtype=jnp.int32)
    is_member = jnp.any(
        (pair_ids * 2 + small_side)[:, None] == leaf_id[None, :], axis=0
    )
    pair = jnp.where(is_member, leaf_id // 2, pair_count).astype(jnp.bfloat16)
    vals = jnp.stack([gradient, hessian, pair, jnp.zeros_like(gradient)])
    local_hist, gains, best = histogram(words, vals, pair_count, bin_count, m)
    feature_gain = gains.reshape(-1, pair_count)
    best_gain = jnp.max(best.reshape(-1, pair_count), axis=0)
    return (local_hist, parent_hist - local_hist, feature_gain, best_gain)


def solution(mesh):
    placed = (
        P("rows", "feat"),
        P("rows"),
        P("rows"),
        P("rows"),
        P(),
        P(("feat", "rows"), None, None),
    )
    return jax.shard_map(
        on_device,
        mesh=mesh,
        in_specs=placed,
        out_specs=(
            P(("feat", "rows"), None, None),
            P(("feat", "rows"), None, None),
            P(("feat", "rows"), None),
            P(),
        ),
        check_vma=False,
    )
```
